32 devices in a mesh: angle: 2 (over y), ty: 8 (over z, core), tx: 2 (over x).
Axes of the slice: x: 2, y: 2, z: 4, core: 2. Of those that a mesh axis runs over, the one named last changes fastest.
Arguments:
- object_slices: float32 [2, 2, 2048, 2048], P('angle', None, 'ty', 'tx'), may hold values from -5 to 5
- probe_field: float32 [2, 256, 256], replicated, may hold values from -6 to 6
- positions: int32 [2, 8, 2, 4, 2], P('angle', 'ty', 'tx'), may hold values from 0 to 1792, as said below
- live_slots: int32 [2, 8, 2], P('angle', 'ty', 'tx'), may hold values from 1 to 4, as said below
- photon_counts: int32 [2, 8, 2, 4, 256, 256], P('angle', 'ty', 'tx'), may hold values from 1 to 1600
Outputs:
- new_object: float32 [2, 2, 2048, 2048], P('angle', None, 'ty', 'tx')
- new_probe: float32 [2, 256, 256], P(None, 'ty')
The draws below stay inside these ranges and needn't reach their ends.
Inputs may be any that keep to these rules, and one draw needn't show every extreme that they name: `positions`: A slot's patch lies inside the object and its centre (top-left plus 128) lies in the rows and columns of the tile that holds the slot: rows r * 256 to (r + 1) * 256 - 1, columns c * 1024 to (c + 1) * 1024 - 1. `live_slots`: some tile of every draw uses all 4 slots.
All inputs are finite; a program needn't handle non-finite values.
Results may differ from the reference program's by a relative error of at most 0.0003.
Values sent between devices are 32-bit elements; how exact they have to be, the bound alone decides.
No kernel may reach another device: no remote copies, remote signals or barrier semaphores. Data moves between devices by JAX's collectives and lax.ppermute only.
A program may use at most 128 MiB of HBM per device.

```python
import jax
import jax.numpy as jnp
from jax import lax

P_SIZE = 256
TR = 256
TC = 1024
SLOTS = 4
ANGLES = 2
NR = 2048
NC = 2048
N_TY = 8
N_TX = 2


def draw_positions(key, part):
    shape = (ANGLES, N_TY, N_TX, SLOTS)
    first_key, second_key = jax.random.split(jax.random.fold_in(key, 11))
    row_draw = jax.random.randint(first_key, shape, 0, TR)
    col_draw = jax.random.randint(second_key, shape, 0, TC)
    tile_row = lax.broadcasted_iota(jnp.int32, shape, 1)
    tile_col = lax.broadcasted_iota(jnp.int32, shape, 2)
    row_start = jnp.clip(tile_row * TR - P_SIZE // 2 + row_draw, 0, NR - P_SIZE)
    col_start = jnp.clip(tile_col * TC - P_SIZE // 2 + col_draw, 0, NC - P_SIZE)
    return jnp.stack([row_start, col_start], axis=-1).astype(jnp.int32)


def draw_live_slots(key, part):
    shape = (ANGLES, N_TY, N_TX)
    first_key, second_key, third_key = jax.random.split(jax.random.fold_in(key, 23), 3)
    sparse = jax.random.randint(first_key, shape, 1, max(SLOTS // 4, 1) + 1)
    dense = jax.random.randint(second_key, shape, 0, 8) == 0
    values = jnp.where(dense, SLOTS, sparse).reshape(-1)
    chosen = jax.random.randint(third_key, (), 0, ANGLES * N_TY * N_TX)
    values = jnp.where(jnp.arange(ANGLES * N_TY * N_TX) == chosen, SLOTS, values)
    return values.reshape(shape).astype(jnp.int32)


def set_ends(result, own_key, smallest, high):
    longest = result.shape.index(max(result.shape))
    spots = []
    for shift in (0, 1):
        where = [jax.random.randint(jax.random.fold_in(own_key, axis), (), 0, length) for axis, length in enumerate(result.shape)]
        where[longest] = (where[longest] + shift) % result.shape[longest]
        spots.append(tuple(where))
    return result.at[spots[0]].set(smallest).at[spots[1]].set(high)


def block_scale(stream_key, shape, cuts, smallest, largest):
    level, own = 1.0, jax.random.fold_in(stream_key, 6)
    for axis_at, parts in cuts:
        draws = jnp.exp(jax.random.uniform(jax.random.fold_in(own, axis_at), (parts,), jnp.float32, smallest / len(cuts), largest / len(cuts)))
        level = level * jnp.repeat(draws, shape[axis_at] // parts).reshape([-1 if axis == axis_at else 1 for axis in range(len(shape))])
    return level


def noise(stream_key, extent, width, limit, pieces=(), kind=jnp.bfloat16):
    gain = block_scale(stream_key, extent, pieces, -0.22, 0.18) if pieces else 1.0
    values = jax.random.normal(stream_key, extent, jnp.float32) * width * gain
    return jnp.minimum(jnp.maximum(values, -limit), limit).astype(kind)


def setup_inputs(seed: int = 0) -> dict:
    key_of = jax.random.split(jax.random.key(seed), 6)
    object_slices = noise(key_of[0], (ANGLES, 2, NR, NC), 0.7, 5.0, ((0, 2), (2, 8), (3, 2)), jnp.float32)
    probe_field = noise(key_of[1], (2, P_SIZE, P_SIZE), 1.0, 6.0, (), jnp.float32)
    positions = draw_positions(jax.random.fold_in(key_of[5], 71), 0)
    live_slots = draw_live_slots(jax.random.fold_in(key_of[5], 71), 0)
    photon_counts = set_ends(jax.random.randint(key_of[4], (ANGLES, N_TY, N_TX, SLOTS, P_SIZE, P_SIZE), 1, 1601), jax.random.fold_in(key_of[4], 1), 1, 1600).astype(jnp.int32)
    return {"object_slices": object_slices, "probe_field": probe_field, "positions": positions, "live_slots": live_slots, "photon_counts": photon_counts}


def reference(object_slices, probe_field, positions, live_slots, photon_counts):
    ftype = object_slices.dtype
    probe_wave = lax.complex(probe_field[0], probe_field[1])
    probe_power = probe_field[0] * probe_field[0] + probe_field[1] * probe_field[1]
    slot_index = jnp.arange(SLOTS, dtype=jnp.int32)
    probe_num = jnp.zeros((P_SIZE, P_SIZE), probe_wave.dtype)
    probe_den = jnp.zeros((P_SIZE, P_SIZE), ftype)
    numerators = []
    denominators = []
    fields = []
    for angle_index in range(ANGLES):
        field = lax.complex(object_slices[angle_index, 0], object_slices[angle_index, 1])
        spots = positions[angle_index].reshape(-1, 2).astype(jnp.int32)
        weights = (slot_index[None, None, :] < live_slots[angle_index][:, :, None]).astype(ftype).reshape(-1)
        measured = photon_counts[angle_index].reshape(-1, P_SIZE, P_SIZE)

        def deposit(carry, item):
            obj_num, obj_den, pr_num, pr_den = carry
            spot, weight, count = item
            row_at = spot[0].astype(jnp.int32)
            col_at = spot[1].astype(jnp.int32)
            patch = lax.dynamic_slice(field, (row_at, col_at), (P_SIZE, P_SIZE))
            wave = probe_wave * patch
            far = jnp.fft.fft2(wave, norm='ortho')
            amplitude = 0.05 * jnp.sqrt(count.astype(ftype))
            factor = amplitude * lax.rsqrt(jnp.maximum(far.real * far.real + far.imag * far.imag, 0.0625))
            gap = (jnp.fft.ifft2(far * factor, norm='ortho') - wave) * weight
            current = lax.dynamic_slice(obj_num, (row_at, col_at), (P_SIZE, P_SIZE))
            obj_num = lax.dynamic_update_slice(obj_num, current + jnp.conj(probe_wave) * gap, (row_at, col_at))
            current_den = lax.dynamic_slice(obj_den, (row_at, col_at), (P_SIZE, P_SIZE))
            obj_den = lax.dynamic_update_slice(obj_den, current_den + weight * probe_power, (row_at, col_at))
            pr_num = pr_num + jnp.conj(patch) * gap
            pr_den = pr_den + weight * (patch.real * patch.real + patch.imag * patch.imag)
            return ((obj_num, obj_den, pr_num, pr_den), None)
        start = (jnp.zeros(field.shape, field.dtype), jnp.zeros(field.shape, ftype), probe_num, probe_den)
        (obj_num, obj_den, probe_num, probe_den), _ = lax.scan(deposit, start, (spots, weights, measured))
        numerators.append(obj_num)
        denominators.append(obj_den)
        fields.append(field)
    peak_obj = jnp.max(jnp.stack([jnp.max(den) for den in denominators]))
    peak_probe = jnp.max(probe_den)
    updated = []
    for angle_index in range(ANGLES):
        value = fields[angle_index] + numerators[angle_index] / (denominators[angle_index] + 0.1 * peak_obj)
        updated.append(jnp.stack([value.real, value.imag]))
    new_object = jnp.stack(updated)
    probe_new = probe_wave + probe_num / (probe_den + 0.1 * peak_probe)
    new_probe = jnp.stack([probe_new.real, probe_new.imag])
    return (new_object, new_probe)
```

```python
import functools

import jax
import jax.numpy as jnp
import numpy as np
from jax import lax
from jax.experimental import pallas as pl
from jax.experimental.pallas import tpu as pltpu
from jax.sharding import PartitionSpec as P

LANE = 128
F32 = jnp.float32
BF16 = jnp.bfloat16


def dft_tables(n):
    ids = np.arange(n)
    phase = 2.0 * np.pi / n * (np.outer(ids, ids) % n)
    out = []
    for table in (np.cos(phase) / np.sqrt(n), np.sin(phase) / np.sqrt(n)):
        high = table.astype(jnp.bfloat16)
        rest = (table - high.astype(np.float64)).astype(jnp.bfloat16)
        out += [high, rest]
    return np.stack(out)


def dot(a, b):
    return lax.dot_general(a, b, (((1,), (0,)), ((), ())), preferred_element_type=F32)


def halves(x):
    high = x.astype(BF16)
    return high, (x - high.astype(F32)).astype(BF16)


def dot_table_left(th, tl, x):
    xh, xl = halves(x)
    return dot(th, xh) + (dot(tl, xh) + dot(th, xl))


def dot_table_right(x, th, tl):
    xh, xl = halves(x)
    return dot(xh, th) + (dot(xh, tl) + dot(xl, th))


def copy_all(copies):
    for c in copies:
        c.start()
    for c in copies:
        c.wait()


class Geometry:
    def __init__(self, size, rows, cols, sides):
        self.size = size
        self.half = size // 2
        self.rows, self.cols = rows, cols
        self.blocks = cols // LANE
        self.edge = self.half // LANE
        self.wide_rows = rows + 2 * self.half
        self.wide_blocks = self.blocks + 2 * self.edge
        self.sides = sides

    def piece_shapes(self, channels):
        h, w = self.half, self.edge * LANE
        out = [(channels, self.rows, self.cols), (channels, h, self.cols), (channels, h, self.cols)]
        for _ in range(self.sides):
            out += [(channels, self.rows, w), (channels, h, w), (channels, h, w)]
        return out

    def piece_windows(self, margin):
        h, r = self.half, self.rows
        out = [(h, r, self.edge, self.blocks), (0, h, self.edge, self.blocks), (h + r, h, self.edge, self.blocks)]
        for s in range(self.sides):
            out += [(h, r, margin[s], self.edge), (0, h, margin[s], self.edge), (h + r, h, margin[s], self.edge)]
        return out


def piece_copies(geo, wide, pieces, margin, channels, sems, to_wide, first=0):
    copies = []
    for piece, (row, rows, block, count) in zip(pieces, geo.piece_windows(margin)):
        for ch in range(channels):
            for b in range(count):
                inside = wide.at[ch * geo.wide_blocks + block + b, pl.ds(row, rows), :]
                outside = piece.at[ch, :, pl.ds(b * LANE, LANE)]
                src, dst = (outside, inside) if to_wide else (inside, outside)
                copies.append(pltpu.make_async_copy(src, dst, sems.at[first + len(copies)]))
    return copies


def copy_count(geo, channels):
    return sum(channels * (s[2] // LANE) for s in geo.piece_shapes(channels))


def shifted_out(ref, geo, ch, row, col):
    n = geo.size
    shift = lax.rem(col, LANE)
    block = ch * geo.wide_blocks + lax.div(col, LANE)
    rolled = [
        pltpu.roll(ref[block + i, pl.ds(row, n), :], LANE - shift, 1) for i in range(n // LANE + 1)
    ]
    lane = lax.broadcasted_iota(jnp.int32, (n, LANE), 1)
    return jnp.concatenate(
        [jnp.where(lane < LANE - shift, rolled[i], rolled[i + 1]) for i in range(n // LANE)], axis=1
    )


def add_at(ref, geo, ch, row, col, value):
    n = geo.size
    shift = lax.rem(col, LANE)
    block = ch * geo.wide_blocks + lax.div(col, LANE)
    lane = lax.broadcasted_iota(jnp.int32, (n, LANE), 1)
    rolled = [pltpu.roll(value[:, i * LANE : (i + 1) * LANE], shift, 1) for i in range(n // LANE)]
    count = n // LANE
    for i in range(count + 1):
        low = rolled[i - 1] if i > 0 else jnp.zeros((n, LANE), F32)
        high = rolled[i] if i < count else jnp.zeros((n, LANE), F32)
        where = (block + i, pl.ds(row, n), slice(None))
        ref[where] = ref[where] + jnp.where(lane >= shift, high, low)


def own_den_body(geo, slots, info, probe, *refs):
    pieces = refs[: 3 + 3 * geo.sides]
    wide, sems = refs[3 + 3 * geo.sides :]
    wide[...] = jnp.zeros_like(wide)
    power = probe[0] * probe[0] + probe[1] * probe[1]
    margin = [info[2 * slots + 1 + s] for s in range(geo.sides)]

    @pl.loop(0, slots)
    def _(s):
        @pl.when(s < info[2 * slots])
        def _():
            add_at(wide, geo, 0, info[s], info[slots + s], power)

    copy_all(piece_copies(geo, wide, pieces, margin, 1, sems, False))


def update_body(geo, slots, groups, info, probe, tables, counts, *refs):
    n = geo.size
    k = 3 + 3 * geo.sides
    inputs, outs = refs[:k], refs[k : 2 * k]
    keep, send, wide, acc, sums, cnt, fwd_h, fwd_l, inv_h, inv_l, sems_in, sems_out, sems_cnt = refs[2 * k :]
    margin = [info[2 * slots + 1 + s] for s in range(geo.sides)]
    core = info[2 * slots + 1 + geo.sides]
    loads = piece_copies(geo, wide, inputs, margin, 2, sems_in, True)
    for c in loads:
        c.start()
    fetch = [pltpu.make_async_copy(counts.at[s], cnt.at[s], sems_cnt.at[s]) for s in range(slots)]
    for c in fetch:
        c.start()
    for part, (fwd, inv) in enumerate(((fwd_h, inv_h), (fwd_l, inv_l))):
        cos, sin = tables[part], tables[2 + part]
        fwd[:n, :n] = cos
        fwd[n:, n:] = cos
        fwd[:n, n:] = sin
        fwd[n:, :n] = -sin
        inv[:n, :n] = cos
        inv[n:, n:] = cos
        inv[:n, n:] = -sin
        inv[n:, :n] = sin
    acc[...] = jnp.zeros_like(acc)
    sums[...] = jnp.zeros_like(sums)
    for c in loads:
        c.wait()
    for c in fetch:
        c.wait()

    @pl.loop(0, slots)
    def _(s):
        @pl.when(s < info[2 * slots])
        def _():
            row, col = info[s], info[slots + s]
            xr = shifted_out(wide, geo, 0, row, col)
            xi = shifted_out(wide, geo, 1, row, col)
            qr, qi = probe[0], probe[1]
            er = qr * xr - qi * xi
            ei = qr * xi + qi * xr
            mid = dot_table_left(fwd_h[...], fwd_l[...], jnp.concatenate([er, ei], axis=0))
            far = dot_table_right(
                jnp.concatenate([mid[:n], mid[n:]], axis=1), inv_h[...], inv_l[...]
            )
            fr, fi = far[:, :n], far[:, n:]
            amp = 0.05 * jnp.sqrt(cnt[s].astype(F32))
            factor = amp * lax.rsqrt(jnp.maximum(fr * fr + fi * fi, 0.0625))
            back = dot_table_right(
                jnp.concatenate([fr * factor, fi * factor], axis=1), fwd_h[...], fwd_l[...]
            )
            near = dot_table_left(
                inv_h[...], inv_l[...], jnp.concatenate([back[:, :n], back[:, n:]], axis=0)
            )
            dr = near[:n] - er
            di = near[n:] - ei
            add_at(acc, geo, 0, row, col, qr * dr + qi * di)
            add_at(acc, geo, 1, row, col, qr * di - qi * dr)
            sums[0] += xr * dr + xi * di
            sums[1] += xr * di - xi * dr
            sums[2] += xr * xr + xi * xi

    copies = piece_copies(geo, acc, outs, margin, 2, sems_out, False)
    base = len(copies)
    share = n // (2 * groups)
    for g in range(groups):
        for j, (dst, part) in enumerate(((keep, core), (send, 1 - core))):
            start = pl.multiple_of((2 * g + part) * share, 8)
            copies.append(
                pltpu.make_async_copy(
                    sums.at[:, pl.ds(start, share), :], dst.at[g], sems_out.at[base + 2 * g + j]
                )
            )
    copy_all(copies)


def den_body(geo, edges, *refs):
    k = 3 + 3 * geo.sides
    pieces = refs[:k]
    total, peak = refs[k:]
    h, w = geo.half, geo.edge * LANE
    total[...] = pieces[0][0]
    total[:h] += pieces[1][0]
    total[geo.rows - h :] += pieces[2][0]
    for s in range(geo.sides):
        at = pl.multiple_of(edges[s] * LANE, LANE)
        mid, top, low = pieces[3 + 3 * s : 6 + 3 * s]
        total[:, pl.ds(at, w)] += mid[0]
        total[:h, pl.ds(at, w)] += top[0]
        total[geo.rows - h :, pl.ds(at, w)] += low[0]
    peak[...] = jnp.full(peak.shape, jnp.max(total[...]))


def final_body(geo, edges, peak, tile, den, *refs):
    k = 3 + 3 * geo.sides
    pieces = refs[:k]
    out, num = refs[k:]
    h, w = geo.half, geo.edge * LANE
    scale = 1.0 / (den[...] + 0.1 * peak[0])
    for ch in range(2):
        num[...] = pieces[0][ch]
        num[:h] += pieces[1][ch]
        num[geo.rows - h :] += pieces[2][ch]
        for s in range(geo.sides):
            at = pl.multiple_of(edges[s] * LANE, LANE)
            mid, top, low = pieces[3 + 3 * s : 6 + 3 * s]
            num[:, pl.ds(at, w)] += mid[ch]
            num[:h, pl.ds(at, w)] += top[ch]
            num[geo.rows - h :, pl.ds(at, w)] += low[ch]
        out[ch] = tile[ch] + num[...] * scale


VMEM = pl.BlockSpec(memory_space=pltpu.VMEM)
SMEM = pl.BlockSpec(memory_space=pltpu.SMEM)
ANY = pl.BlockSpec(memory_space=pl.ANY)


def shape_of(*shape):
    return jax.ShapeDtypeStruct(shape, F32)


def call(body, name, outs, ins, in_specs, out_specs, scratch=()):
    return pl.pallas_call(
        body,
        name=name,
        out_shape=outs,
        in_specs=in_specs,
        out_specs=out_specs,
        scratch_shapes=list(scratch),
        compiler_params=pltpu.CompilerParams(vmem_limit_bytes=60000 * 1024),
    )(*ins)


def body(n_angle, n_ty, n_tx, object_slices, probe_field, positions, live_slots, photon_counts):
    size = probe_field.shape[1]
    tile = object_slices[0]
    rows, cols = tile.shape[1], tile.shape[2]
    sides = 0 if n_tx == 1 else 1 if n_tx == 2 else 2
    geo = Geometry(size, rows, cols, sides)
    half, width = geo.half, geo.edge * LANE
    ty, tx = lax.axis_index("ty"), lax.axis_index("tx")
    spots = positions[0, 0, 0]
    slots = spots.shape[0]
    if sides == 1:
        margin = [jnp.where(tx == 0, geo.wide_blocks - geo.edge, 0)]
        edges = [jnp.where(tx == 0, geo.blocks - geo.edge, 0)]
    else:
        margin = [0, geo.wide_blocks - geo.edge][:sides]
        edges = [0, geo.blocks - geo.edge][:sides]
    info = jnp.concatenate(
        [
            spots[:, 0] - (ty * rows - half),
            spots[:, 1] - (tx * cols - half),
            live_slots[0, 0],
            jnp.stack([jnp.asarray(m, jnp.int32) for m in margin + [ty % 2]]),
        ]
    ).astype(jnp.int32)
    edge_info = jnp.stack([jnp.asarray(e, jnp.int32) for e in edges + [0]]).astype(jnp.int32)

    def move(x, dty, dtx):
        pairs = []
        for r in range(n_ty):
            for c in range(n_tx):
                to_r, to_c = r + dty, (1 - c) if dtx is None else c + dtx
                if 0 <= to_r < n_ty and 0 <= to_c < n_tx:
                    pairs.append((r * n_tx + c, to_r * n_tx + to_c))
        return lax.ppermute(x, ("ty", "tx"), pairs)

    def swap_sides(sends, dty):
        if sides == 1:
            return [move(sends[0], dty, None)]
        if sides == 2:
            return [move(sends[1], dty, 1), move(sends[0], dty, -1)]
        return []

    def exchange(up, down, side, side_up, side_down):
        above = move(down, 1, 0)
        below = move(up, -1, 0)
        mids = swap_sides(side, 0)
        tops = swap_sides(side_down, 1)
        lows = swap_sides(side_up, -1)
        out = [above, below]
        for s in range(sides):
            out += [mids[s], tops[s], lows[s]]
        return out

    def edge_columns(x):
        return [lax.dynamic_slice_in_dim(x, jnp.asarray(e, jnp.int32) * LANE, width, 2) for e in edges]

    strips = edge_columns(tile)
    halos = exchange(
        tile[:, :half],
        tile[:, rows - half :],
        strips,
        [s[:, :half] for s in strips],
        [s[:, rows - half :] for s in strips],
    )

    def pieces_of(channels):
        return [shape_of(*s) for s in geo.piece_shapes(channels)]

    pieces = 3 + 3 * sides
    own_den = call(
        functools.partial(own_den_body, geo, slots),
        "own_den",
        pieces_of(1),
        (info, probe_field),
        [SMEM, VMEM],
        [ANY] * pieces,
        [
            pltpu.VMEM((geo.wide_blocks, geo.wide_rows, LANE), F32),
            pltpu.SemaphoreType.DMA((copy_count(geo, 1),)),
        ],
    )

    def spread(p):
        return exchange(p[1], p[2], p[3::3], p[4::3], p[5::3])

    den_halos = spread(own_den)

    groups = n_ty // 2
    share = size // n_ty
    n_copies = copy_count(geo, 2)
    wide = pltpu.VMEM((2 * geo.wide_blocks, geo.wide_rows, LANE), F32)
    table = pltpu.VMEM((2 * size, 2 * size), BF16)
    updates = call(
        functools.partial(update_body, geo, slots, groups),
        "update",
        pieces_of(2) + [shape_of(groups, 3, share, size)] * 2,
        (info, probe_field, jnp.asarray(dft_tables(size)), photon_counts[0, 0, 0], tile, *halos),
        [SMEM, VMEM, VMEM, ANY] + [ANY] * pieces,
        [ANY] * (pieces + 2),
        [wide, wide, pltpu.VMEM((3, size, size), F32), pltpu.VMEM((slots, size, size), jnp.int32)]
        + [table] * 4
        + [
            pltpu.SemaphoreType.DMA((n_copies,)),
            pltpu.SemaphoreType.DMA((n_copies + 2 * groups,)),
            pltpu.SemaphoreType.DMA((slots,)),
        ],
    )
    num, keep, send = updates[:pieces], updates[-2], updates[-1]
    num_halos = spread(num)

    den, peak_tile = call(
        functools.partial(den_body, geo),
        "den",
        [shape_of(rows, cols), shape_of(8, LANE)],
        (edge_info, own_den[0], *den_halos),
        [SMEM] + [VMEM] * pieces,
        [VMEM, VMEM],
    )

    def pairs_xor(count, bit):
        return [(i, i ^ bit) for i in range(count)]

    def sum_scatter_ty(keep, send):
        part = keep + lax.ppermute(send, "ty", pairs_xor(n_ty, 1))
        mine = ty // 2
        total = lax.dynamic_index_in_dim(part, mine, 0, keepdims=False)
        for step in range(1, groups):
            if groups & (groups - 1) == 0:
                target = mine ^ step
                pairs = pairs_xor(n_ty, 2 * step)
            else:
                target = (mine + step) % groups
                pairs = [(i, (i + 2 * step) % n_ty) for i in range(n_ty)]
            piece = lax.dynamic_index_in_dim(part, target, 0, keepdims=False)
            total = total + lax.ppermute(piece, "ty", pairs)
        return total

    def all_combine(x, axis, op):
        count = {"angle": n_angle, "ty": n_ty, "tx": n_tx}[axis]
        if count & (count - 1) == 0:
            bit = 1
            while bit < count:
                x = op(x, lax.ppermute(x, axis, pairs_xor(count, bit)))
                bit *= 2
            return x
        return (lax.psum if op is jnp.add else lax.pmax)(x, axis)

    def combine_plane(x, op):
        if n_angle * n_tx == 4 and n_tx == 2:
            got = [lax.ppermute(x, ("angle", "tx"), pairs_xor(4, bit)) for bit in (1, 2, 3)]
            return op(op(x, got[0]), op(got[1], got[2]))
        return all_combine(all_combine(x, "angle", op), "tx", op)

    sums = combine_plane(sum_scatter_ty(keep, send), jnp.add)
    peaks = jnp.stack([peak_tile[0, 0], jnp.max(sums[2])])
    peaks = all_combine(combine_plane(peaks, jnp.maximum), "ty", jnp.maximum)

    new_tile = call(
        functools.partial(final_body, geo),
        "final",
        shape_of(2, rows, cols),
        (edge_info, peaks, tile, den, num[0], *num_halos),
        [SMEM, SMEM] + [VMEM] * (2 + pieces),
        VMEM,
        [pltpu.VMEM((rows, cols), F32)],
    )
    scale = 1.0 / (sums[2] + 0.1 * peaks[1])
    probe_rows = lax.dynamic_slice_in_dim(probe_field, ty * share, share, 1)
    return new_tile[None], probe_rows + sums[:2] * scale[None]


def solution(mesh):
    sizes = dict(mesh.shape)
    return jax.shard_map(
        functools.partial(body, sizes["angle"], sizes["ty"], sizes["tx"]),
        mesh=mesh,
        in_specs=(
            P("angle", None, "ty", "tx"),
            P(),
            P("angle", "ty", "tx", None, None),
            P("angle", "ty", "tx"),
            P("angle", "ty", "tx", None, None, None),
        ),
        out_specs=(P("angle", None, "ty", "tx"), P(None, "ty", None)),
        check_vma=False,
    )
```
